32 devices in a mesh: shard: 8 (over z, y), width: 4 (over x, core).
Axes of the slice: x: 2, y: 2, z: 4, core: 2. Of those that a mesh axis runs over, the one named last changes fastest.
Arguments:
- one_query: float32 [3584, 4096], P('shard', 'width'), may hold values from -0.125 to 0.125
- other_query: float32 [3584, 4096], P('shard', 'width'), may hold values from -0.09375 to 0.09375
- one_key: float32 [3584, 2048], P('shard', 'width'), may hold values from -0.125 to 0.125
- other_key: float32 [3584, 2048], P('shard', 'width'), may hold values from -0.09375 to 0.09375
- one_value: float32 [3584, 2048], P('shard', 'width'), may hold values from -0.125 to 0.125
- other_value: float32 [3584, 2048], P('shard', 'width'), may hold values from -0.09375 to 0.09375
- mix_share: float32 [3584], P('shard'), may hold values from 0.2 to 0.8
- norm_gain: float32 [3584], P('shard'), may hold values from 0.25 to 1.75
Outputs:
- final_query: bfloat16 [3584, 4096], P(None, 'width')
- final_key: bfloat16 [3584, 2048], P(None, 'width')
- final_value: bfloat16 [3584, 2048], P(None, 'width')
- scale_query: float32 [4096], P('width')
- scale_key: float32 [2048], P('width')
- scale_value: float32 [2048], P('width')
The draws below stay inside these ranges and needn't reach their ends.
All inputs are finite; a program needn't handle non-finite values.
Results may differ from the reference program's by a relative error of at most 0.001.
Values may be sent and summed in bfloat16 or wider, within the bound.
No kernel may reach another device: no remote copies, remote signals or barrier semaphores. Data moves between devices by JAX's collectives and lax.ppermute only.
A program may use at most 128 MiB of HBM per device.

```python
import jax
import jax.numpy as jnp
from jax import lax

D_MODEL = 3584
Q_DIM = 4096
KV_DIM = 2048


def raised(array, own_key, source, target, blocks, factor):
    def block_of(axis_at):
        return (jnp.arange(array.shape[axis_at]) // (array.shape[axis_at] // blocks)).reshape((-1,) + (1,) * (array.ndim - 1 - axis_at))

    first = jax.random.permutation(own_key, blocks)[block_of(target)]
    second = (block_of(target) + blocks // 2) % blocks
    return jnp.where((block_of(source) == first) | (block_of(source) == second), factor * array, array)


def shard_levels(own_key, dims, cuts, low, top_value):
    loudness, own = 1.0, jax.random.fold_in(own_key, 6)
    for position, parts in cuts:
        draws = jnp.exp(jax.random.uniform(jax.random.fold_in(own, position), (parts,), jnp.float32, low / len(cuts), top_value / len(cuts)))
        loudness = loudness * jnp.repeat(draws, dims[position] // parts).reshape([-1 if axis == position else 1 for axis in range(len(dims))])
    return loudness


def normal_values(rng, shape, width, most, pieces=(), dtype=jnp.bfloat16):
    factor_of = shard_levels(rng, shape, pieces, -0.22, 0.18) if pieces else 1.0
    result = jax.random.normal(rng, shape, jnp.float32) * width * factor_of
    return jnp.minimum(jnp.maximum(result, -most), most).astype(dtype)


def bell_draw_with(own_key, extent, scale, most, cuts, heavy, kind=jnp.bfloat16):
    values = scale * jax.random.normal(own_key, extent, jnp.float32)
    if cuts:
        values = values * shard_levels(own_key, extent, cuts, -0.22, 0.18)
    return jnp.clip(raised(values, jax.random.fold_in(own_key, 3), *heavy), -most, most).astype(kind)


def setup_inputs(seed: int = 0) -> dict:
    key_list = jax.random.split(jax.random.key(seed), 9)
    one_query = bell_draw_with(key_list[0], (D_MODEL, Q_DIM), D_MODEL ** -0.5, 0.125, ((0, 8), (1, 4)), (0, 1, 8, 2.0), jnp.float32)
    other_query = normal_values(key_list[1], (D_MODEL, Q_DIM), D_MODEL ** -0.5, 0.09375, ((0, 8), (1, 4)), jnp.float32)
    one_key = bell_draw_with(key_list[2], (D_MODEL, KV_DIM), D_MODEL ** -0.5, 0.125, ((0, 8), (1, 4)), (0, 1, 8, 2.0), jnp.float32)
    other_key = normal_values(key_list[3], (D_MODEL, KV_DIM), D_MODEL ** -0.5, 0.09375, ((0, 8), (1, 4)), jnp.float32)
    one_value = bell_draw_with(key_list[4], (D_MODEL, KV_DIM), D_MODEL ** -0.5, 0.125, ((0, 8), (1, 4)), (0, 1, 8, 2.0), jnp.float32)
    other_value = normal_values(key_list[5], (D_MODEL, KV_DIM), D_MODEL ** -0.5, 0.09375, ((0, 8), (1, 4)), jnp.float32)
    mix_share = jnp.clip(0.2 + 0.6 * jax.random.uniform(key_list[6], (D_MODEL,), jnp.float32) ** shard_levels(key_list[6], (D_MODEL,), ((0, 8),), -0.2, 0.2), 0.2, 0.8)
    norm_gain = jnp.clip(1.0 + 0.15 * jax.random.normal(key_list[7], (D_MODEL,), jnp.float32), 0.25, 1.75)
    return {"one_query": one_query, "other_query": other_query, "one_key": one_key, "other_key": other_key, "one_value": one_value, "other_value": other_value, "mix_share": mix_share, "norm_gain": norm_gain}


def reference(one_query, other_query, one_key, other_key, one_value, other_value, mix_share, norm_gain):
    result_query = mix_share[:, None] * one_query + (1.0 - mix_share[:, None]) * other_query
    result_key = mix_share[:, None] * one_key + (1.0 - mix_share[:, None]) * other_key
    result_value = mix_share[:, None] * one_value + (1.0 - mix_share[:, None]) * other_value
    result_gained_query = result_query * norm_gain[:, None]
    result_gained_key = result_key * norm_gain[:, None]
    result_gained_value = result_value * norm_gain[:, None]
    scale_query = jnp.sqrt(lax.optimization_barrier(jnp.sum(result_gained_query * result_gained_query, axis=0)))
    final_query = (result_gained_query / scale_query).astype(jnp.bfloat16)
    scale_key = jnp.sqrt(lax.optimization_barrier(jnp.sum(result_gained_key * result_gained_key, axis=0)))
    final_key = (result_gained_key / scale_key).astype(jnp.bfloat16)
    scale_value = jnp.sqrt(lax.optimization_barrier(jnp.sum(result_gained_value * result_gained_value, axis=0)))
    final_value = (result_gained_value / scale_value).astype(jnp.bfloat16)
    return (final_query, final_key, final_value, scale_query, scale_key, scale_value)
```

```python
import jax
import jax.numpy as jnp
from jax import lax
from jax.sharding import PartitionSpec as P

AXIS = "shard"


def ring_order(n):
    if n % 2:
        return list(range(n))
    return list(range(0, n, 2)) + list(range(n - 1, 0, -2))


def tree(parts):
    while len(parts) > 1:
        pairs = [parts[i] + parts[i + 1] for i in range(0, len(parts) - 1, 2)]
        parts = pairs + ([parts[-1]] if len(parts) % 2 else [])
    return parts[0]


def all_sum(x, n):
    if n & (n - 1):
        return lax.psum(x, AXIS)
    done = 1
    while done < n:
        width = min(8, n // done)
        parts = [x]
        for k in range(1, width):
            parts.append(lax.ppermute(x, AXIS, [(i, i ^ (k * done)) for i in range(n)]))
        x = tree(parts)
        done *= width
    return x


def mixed(one, other, share, gain):
    return (share * one + (1.0 - share) * other) * gain


def make_body(n):
    order = ring_order(n)
    position = [order.index(i) for i in range(n)]
    forward = [(order[i], order[(i + 1) % n]) for i in range(n)]
    backward = [(b, a) for a, b in forward]

    def body(one_query, other_query, one_key, other_key, one_value, other_value, mix_share, norm_gain):
        share, gain = mix_share[:, None], norm_gain[:, None]
        query = mixed(one_query, other_query, share, gain)
        key = mixed(one_key, other_key, share, gain)
        value = mixed(one_value, other_value, share, gain)
        rows, q_width = query.shape
        kv_width = key.shape[1]
        local = jnp.concatenate([jnp.sum(a * a, axis=0) for a in (query, key, value)])
        total = all_sum(local.reshape(8, -1), n).reshape(-1)
        scale = jnp.sqrt(total)
        scale_query = scale[:q_width]
        scale_key = scale[q_width : q_width + kv_width]
        scale_value = scale[q_width + kv_width :]
        narrow_query = (query / scale_query).astype(jnp.bfloat16)
        narrow_kv = jnp.stack(
            [(key / scale_key).astype(jnp.bfloat16), (value / scale_value).astype(jnp.bfloat16)]
        )

        me = lax.axis_index(AXIS)
        table = jnp.asarray(
            [[order[(position[i] - h) % n] for h in range(n)] for i in range(n)], jnp.int32
        )
        sources = lax.dynamic_index_in_dim(table, me, 0, keepdims=False)

        outs = [
            jnp.zeros((n, rows, q_width), jnp.bfloat16),
            jnp.zeros((n, rows, kv_width), jnp.bfloat16),
            jnp.zeros((n, rows, kv_width), jnp.bfloat16),
        ]

        def put_query(block, hop):
            outs[0] = lax.dynamic_update_slice(outs[0], block[None], (sources[hop % n], 0, 0))

        def put_kv(block, hop):
            outs[1] = lax.dynamic_update_slice(outs[1], block[:1], (sources[hop % n], 0, 0))
            outs[2] = lax.dynamic_update_slice(outs[2], block[1:], (sources[hop % n], 0, 0))

        put_query(narrow_query, 0)
        put_kv(narrow_kv, 0)
        q_up = q_down = narrow_query
        kv_up = kv_down = narrow_kv
        up_hops, down_hops = n // 2, (n - 1) // 2
        for hop in range(1, up_hops + 1):
            both = hop <= down_hops
            q_up = lax.ppermute(q_up, AXIS, forward)
            kv_down = lax.ppermute(kv_down, AXIS, backward)
            if both:
                kv_up = lax.ppermute(kv_up, AXIS, forward)
                q_down = lax.ppermute(q_down, AXIS, backward)
            put_query(q_up, hop)
            put_kv(kv_down, -hop)
            if both:
                put_kv(kv_up, hop)
                put_query(q_down, -hop)
        final = [a.reshape(n * rows, -1) for a in outs]
        return (*final, scale_query, scale_key, scale_value)

    return body


def solution(mesh):
    cut = P(AXIS, "width")
    return jax.shard_map(
        make_body(mesh.shape[AXIS]),
        mesh=mesh,
        in_specs=(cut,) * 6 + (P(AXIS),) * 2,
        out_specs=(P(None, "width"),) * 3 + (P("width"),) * 3,
        check_vma=False,
    )
```

```python
import jax
import jax.numpy as jnp
from jax import lax
from jax.sharding import PartitionSpec as P

AXIS = "shard"
RING_MOST = 16


def ring_order(n):
    if n % 2:
        return list(range(n))
    return list(range(0, n, 2)) + list(range(n - 1, 0, -2))


def tree(parts):
    while len(parts) > 1:
        pairs = [parts[i] + parts[i + 1] for i in range(0, len(parts) - 1, 2)]
        parts = pairs + ([parts[-1]] if len(parts) % 2 else [])
    return parts[0]


def all_sum(x, n):
    if n & (n - 1) or n > RING_MOST:
        return lax.psum(x, AXIS)
    done = 1
    while done < n:
        width = 2
        parts = [x]
        for k in range(1, width):
            parts.append(lax.ppermute(x, AXIS, [(i, i ^ (k * done)) for i in range(n)]))
        x = tree(parts)
        done *= width
    return x


def mixed(one, other, share, gain):
    return (share * one + (1.0 - share) * other) * gain


def make_body(n):
    order = ring_order(n)
    position = [order.index(i) for i in range(n)]
    forward = [(order[i], order[(i + 1) % n]) for i in range(n)]
    backward = [(b, a) for a, b in forward]

    def body(one_query, other_query, one_key, other_key, one_value, other_value, mix_share, norm_gain):
        share, gain = mix_share[:, None], norm_gain[:, None]
        query = mixed(one_query, other_query, share, gain)
        key = mixed(one_key, other_key, share, gain)
        value = mixed(one_value, other_value, share, gain)
        rows, q_width = query.shape
        kv_width = key.shape[1]
        local = jnp.concatenate([jnp.sum(a * a, axis=0) for a in (query, key, value)])
        total = all_sum(local, n)
        outs = [
            jnp.zeros((n, rows, q_width), jnp.bfloat16),
            jnp.zeros((n, rows, kv_width), jnp.bfloat16),
            jnp.zeros((n, rows, kv_width), jnp.bfloat16),
        ]
        scale = jnp.sqrt(total)
        scale_query = scale[:q_width]
        scale_key = scale[q_width : q_width + kv_width]
        scale_value = scale[q_width + kv_width :]
        narrow_query = (query / scale_query).astype(jnp.bfloat16)
        narrow_kv = jnp.stack(
            [(key / scale_key).astype(jnp.bfloat16), (value / scale_value).astype(jnp.bfloat16)]
        )

        narrow_query = lax.optimization_barrier(narrow_query)
        narrow_kv = lax.optimization_barrier(narrow_kv)
        if n > RING_MOST:
            finals = [
                lax.all_gather(a, AXIS, axis=0, tiled=True) for a in (narrow_query, narrow_kv[0], narrow_kv[1])
            ]
            return (*finals, scale_query, scale_key, scale_value)

        me = lax.axis_index(AXIS)
        table = jnp.asarray(
            [[order[(position[i] - h) % n] for h in range(n)] for i in range(n)], jnp.uint32
        )
        zero = jnp.uint32(0)
        sources = lax.dynamic_index_in_dim(table, me, 0, keepdims=False)

        def put_query(block, hop):
            outs[0] = lax.dynamic_update_slice(outs[0], block[None], (sources[hop % n], zero, zero))

        def put_kv(block, hop):
            outs[1] = lax.dynamic_update_slice(outs[1], block[:1], (sources[hop % n], zero, zero))
            outs[2] = lax.dynamic_update_slice(outs[2], block[1:], (sources[hop % n], zero, zero))

        put_query(narrow_query, 0)
        put_kv(narrow_kv, 0)
        q_up = q_down = narrow_query
        kv_up = kv_down = narrow_kv
        for hop in range(1, (n - 1) // 2 + 1):
            q_up = lax.ppermute(q_up, AXIS, forward)
            q_down = lax.ppermute(q_down, AXIS, backward)
            kv_up = lax.ppermute(kv_up, AXIS, forward)
            kv_down = lax.ppermute(kv_down, AXIS, backward)
            put_query(q_up, hop)
            put_query(q_down, -hop)
            put_kv(kv_up, hop)
            put_kv(kv_down, -hop)
        if n % 2 == 0:
            far, half = sources[n // 2], q_width // 2
            key_up = lax.ppermute(kv_up[:1], AXIS, forward)
            value_down = lax.ppermute(kv_down[1:], AXIS, backward)
            left_up = lax.ppermute(q_up[:, :half], AXIS, forward)
            right_down = lax.ppermute(q_down[:, half:], AXIS, backward)
            outs[1] = lax.dynamic_update_slice(outs[1], key_up, (far, zero, zero))
            outs[2] = lax.dynamic_update_slice(outs[2], value_down, (far, zero, zero))
            outs[0] = lax.dynamic_update_slice(outs[0], left_up[None], (far, zero, zero))
            outs[0] = lax.dynamic_update_slice(outs[0], right_down[None], (far, zero, zero + half))
        final = [a.reshape(n * rows, -1) for a in outs]
        return (*final, scale_query, scale_key, scale_value)

    return body


def solution(mesh):
    cut = P(AXIS, "width")
    return jax.shard_map(
        make_body(mesh.shape[AXIS]),
        mesh=mesh,
        in_specs=(cut,) * 6 + (P(AXIS),) * 2,
        out_specs=(P(None, "width"),) * 3 + (P("width"),) * 3,
        check_vma=False,
    )
```
